32 devices in a mesh: dp: 16 (over z, y, x), tm: 2 (over core).
Axes of the slice: x: 2, y: 2, z: 4, core: 2. Of those that a mesh axis runs over, the one named last changes fastest.
Arguments:
- hidden: bfloat16 [32, 256, 4096], P('dp', 'tm'), may hold values from -6 to 6
- first_weight: bfloat16 [4096, 1024], P('dp'), may hold values from -0.09375 to 0.09375
- first_bias: float32 [1024], replicated, may hold values from -3 to 3
- second_weight: float32 [1024], replicated, may hold values from -0.1875 to 0.1875
- second_bias: float32 [1], replicated, may hold values from -3 to 3
- rewards: float32 [32, 256], P('dp', 'tm'), may hold values from -0.8 to 0.8
- dones: int32 [32, 256], P('dp', 'tm'), may hold values 0 or 1
- lengths: int32 [32], P('dp'), may hold values from 128 to 256
- discount: float32 [32], P('dp'), may hold values from 0.96 to 1
- trace: float32 [32], P('dp'), may hold values from 0.99609375 to 1
Outputs:
- advantages: float32 [32, 256], P('dp', 'tm')
- returns: float32 [32, 256], P('dp', 'tm')
The draws below stay inside these ranges and needn't reach their ends.
All inputs are finite; a program needn't handle non-finite values. No bound on the sum of `dones` on one device may be relied on, other than what follows from the above.
Results may differ from the reference program's by a relative error of at most 0.0003.
Values may be sent and summed in bfloat16 or wider, within the bound.
No kernel may reach another device: no remote copies, remote signals or barrier semaphores. Data moves between devices by JAX's collectives and lax.ppermute only.
A program may use at most 64 MiB of HBM per device.

```python
import jax
import jax.numpy as jnp
from jax import lax

D = 4096
CRITIC = 1024
TRAJ = 32
STEPS = 256


def draw_discount(key, part):
    uniform_draw = jax.random.uniform(jax.random.fold_in(key, 11), (TRAJ,), jnp.float32)
    low_rate = jnp.log(0.3)
    high_rate = jnp.log(STEPS / 25.0)
    rate = jnp.exp(low_rate + uniform_draw * (high_rate - low_rate))
    return jnp.exp(-rate / STEPS).astype(jnp.float32)


def draw_trace(key, part):
    uniform_draw = jax.random.uniform(jax.random.fold_in(key, 23), (TRAJ,), jnp.float32)
    rate = jnp.exp(jnp.log(0.1) + uniform_draw * (jnp.log(1.0) - jnp.log(0.1)))
    return jnp.exp(-rate / STEPS).astype(jnp.float32)


def touch_ends(array, rng, low, largest):
    longest = array.shape.index(max(array.shape))
    spots = []
    for shift in (0, 1):
        where = [jax.random.randint(jax.random.fold_in(rng, axis), (), 0, length) for axis, length in enumerate(array.shape)]
        where[longest] = (where[longest] + shift) % array.shape[longest]
        spots.append(tuple(where))
    return array.at[spots[0]].set(low).at[spots[1]].set(largest)


def block_levels(stream_key, extent, split, least, top_value):
    factor_of, own = 1.0, jax.random.fold_in(stream_key, 6)
    for axis_at, shards_of in split:
        heights = jnp.exp(jax.random.uniform(jax.random.fold_in(own, axis_at), (shards_of,), jnp.float32, least / len(split), top_value / len(split)))
        factor_of = factor_of * jnp.repeat(heights, extent[axis_at] // shards_of).reshape([-1 if axis == axis_at else 1 for axis in range(len(extent))])
    return factor_of


def noise(key, dims, deviation, limit, split=(), kind=jnp.bfloat16):
    level = block_levels(key, dims, split, -0.22, 0.18) if split else 1.0
    entries = jax.random.normal(key, dims, jnp.float32) * deviation * level
    return jnp.minimum(jnp.maximum(entries, -limit), limit).astype(kind)


def setup_inputs(seed: int = 0) -> dict:
    splits = jax.random.split(jax.random.key(seed), 11)
    return {
        "hidden": noise(splits[0], (TRAJ, STEPS, D), 1.0, 6.0, ((0, 16), (1, 2))),
        "first_weight": noise(splits[1], (D, CRITIC), D ** -0.5, 0.09375, ((0, 16),)),
        "first_bias": noise(splits[2], (CRITIC,), 0.5, 3.0, (), jnp.float32),
        "second_weight": noise(splits[3], (CRITIC,), CRITIC ** -0.5, 0.1875, (), jnp.float32),
        "second_bias": noise(splits[4], (1,), 1.0, 3.0, (), jnp.float32),
        "rewards": noise(splits[5], (TRAJ, STEPS), 0.1, 0.8, ((0, 16), (1, 2)), jnp.float32),
        "dones": touch_ends((jax.random.randint(splits[6], (TRAJ, STEPS), 0, 256) < 1).astype(jnp.int32), jax.random.fold_in(splits[6], 1), 0, 1),
        "lengths": touch_ends(jax.random.randint(splits[7], (TRAJ,), STEPS // 2, STEPS + 1), jax.random.fold_in(splits[7], 1), STEPS // 2, STEPS).astype(jnp.int32),
        "discount": draw_discount(jax.random.fold_in(splits[10], 71), 0),
        "trace": draw_trace(jax.random.fold_in(splits[10], 71), 0),
    }


def reference(hidden, first_weight, first_bias, second_weight, second_bias, rewards, dones, lengths, discount, trace):

    def critic_one(trajectory):
        pre = jnp.dot(trajectory, first_weight, preferred_element_type=jnp.float32)
        return jnp.dot(jax.nn.silu(pre + first_bias), second_weight, precision=lax.Precision.HIGHEST) + second_bias[0]
    values = lax.map(critic_one, hidden)
    time_index = jnp.arange(STEPS, dtype=jnp.int32)
    live = (time_index[None, :] < lengths[:, None]).astype(jnp.float32)
    live_next = ((time_index + 1)[None, :] < lengths[:, None]).astype(jnp.float32)
    keep = 1.0 - dones.astype(jnp.float32)
    value_next = jnp.concatenate([values[:, 1:], jnp.zeros((values.shape[0], 1), jnp.float32)], axis=1)
    gamma = discount[:, None]
    delta = live * (rewards + gamma * keep * live_next * value_next - values)
    decay = gamma * trace[:, None] * keep * live_next

    def backward(running, inputs):
        updated = inputs[1] + inputs[0] * running
        return (updated, updated)
    start = jnp.zeros((values.shape[0],), jnp.float32)
    _, gains = lax.scan(backward, start, (decay.T, delta.T), reverse=True)
    gain = gains.T
    returns = live * (gain + values)
    count = jnp.sum(live)
    mean = jnp.sum(gain) / count
    spread = jnp.sum(live * (gain - mean) ** 2) / count
    advantages = live * (gain - mean) / jnp.sqrt(spread + 1e-06)
    return (advantages, returns)
```

```python
import functools

import jax
import jax.numpy as jnp
from jax import lax
from jax.experimental import pallas as pl
from jax.experimental.pallas import tpu as pltpu
from jax.sharding import PartitionSpec as P


BOTH = ("dp", "tm")


def ring_places(count):
    order = [0] + list(range(1, count, 2)) + [r for r in range(count - 1, 0, -1) if r % 2 == 0]
    return order, {r: i for i, r in enumerate(order)}


def routes(dp_size, tm_size):
    order, place = ring_places(dp_size // 4)
    first, second, up, down = [], [], [], []
    for d in range(dp_size):
        plane, q = d // 4, d % 4
        above = order[(place[plane] + 1) % len(order)]
        below = order[(place[plane] - 1) % len(order)]
        for t in range(tm_size):
            here = d * tm_size + t
            a, b = (1, 2) if t % 2 == 0 else (2, 1)
            first.append((here, (d ^ a) * tm_size + t))
            second.append((here, (d ^ b) * tm_size + t))
            up.append((here, (above * 4 + q) * tm_size + t))
            down.append((here, (below * 4 + q) * tm_size + t))
    return first, second, up, down


def passed_along(block, axis, distance):
    devices = range(lax.axis_size(axis))
    route = [(i - distance, i) for i in devices if i - distance in devices]
    return lax.ppermute(block, axis, route)


def pair_combine(earlier, later):
    return (earlier[0] * later[0], later[1] + later[0] * earlier[1])


def moments(gain, live):
    count, total = jnp.sum(live), jnp.sum(gain)
    deviation = live * (gain - total / jnp.maximum(count, 1.0))
    return count, total, jnp.sum(deviation * deviation)


def normalized(every, gain, live):
    counts, totals, squares = every[:, 0:1], every[:, 1:2], every[:, 2:3]
    count = jnp.sum(counts)
    mean = jnp.sum(totals) / count
    shift = totals / jnp.maximum(counts, 1.0) - mean
    spread = jnp.sum(squares + counts * shift * shift) / count
    return live * (gain - mean) / jnp.sqrt(jnp.full(gain.shape, spread + 1e-06))


def core_parity():
    return lax.bitwise_and(lax.axis_index("tm"), 1)


def columns_of(kind, k, planes, shard):
    d, parity = lax.axis_index("dp"), core_parity()
    order, place = ring_places(planes)
    plane, q = lax.shift_right_logical(d, 2), lax.bitwise_and(d, 3)
    source = 0
    for r in range(planes):
        source = jnp.where(plane == r, order[(place[r] - k) % planes], source)
    turns = (0, 1 + parity) if kind == "near" else (2 - parity, 3)
    return [(source * 4 + lax.bitwise_xor(q, turn)) * shard for turn in turns]


def bring_kernel(rows_ref, bias_ref, out_weight_ref, own_ref, constants_ref, sems):
    units = constants_ref.shape[1]
    mine = pl.ds(pl.multiple_of(core_parity() * units, units), units)
    copies = [
        pltpu.make_async_copy(rows_ref, own_ref, sems.at[0]),
        pltpu.make_async_copy(bias_ref.at[:, mine], constants_ref.at[0:1, :], sems.at[1]),
        pltpu.make_async_copy(out_weight_ref.at[:, mine], constants_ref.at[1:2, :], sems.at[2]),
    ]
    for copy in copies:
        copy.start()
    for copy in copies:
        copy.wait()


def dot_kernel(groups, planes, first_call, own_ref, other_ref, *refs):
    pre_ref = refs[-1]
    count = sum(len(x[2]) for x in groups)
    total = None if first_call else refs[count][...]
    taken = 0
    for kind, k, parts in groups:
        shard = refs[taken].shape[0]
        columns = [pl.ds(pl.multiple_of(at, shard), shard) for at in columns_of(kind, k, planes, shard)]
        for part in parts:
            block = jnp.concatenate([own_ref[:, columns[part]], other_ref[:, columns[part]]], axis=0)
            more = jnp.dot(block, refs[taken][...], preferred_element_type=jnp.float32)
            total = more if total is None else total + more
            taken += 1
    pre_ref[...] = total


def value_kernel(groups, planes, own_ref, other_ref, *refs):
    count = sum(len(x[2]) for x in groups)
    constants_ref, part_ref, pre_ref = refs[count + 1 :]
    dot_kernel(groups, planes, False, own_ref, other_ref, *refs[: count + 1], pre_ref)
    rows, units = pre_ref.shape
    bias, out_weight = constants_ref[0:1, :], constants_ref[1:2, :]
    for side in range(2):
        for at in range(0, rows // 2, 128):
            v = pre_ref[side * (rows // 2) + at : side * (rows // 2) + at + 128, :] + bias
            weighted = v / (1.0 + jnp.exp(-v)) * out_weight
            folded = sum(weighted[:, u : u + 128] for u in range(0, units, 128))
            part_ref[side : side + 1, at : at + 128] = jnp.sum(folded.T, axis=0, keepdims=True)


def prepare_kernel(
    rewards_ref, other_rewards_ref, dones_ref, other_dones_ref, lengths_ref, discount_ref, trace_ref, out_bias_ref, ready_ref, own_live_ref
):
    traj, step = rewards_ref.shape
    parity = core_parity()
    early = parity == 0

    def in_time(own, other):
        return jnp.concatenate([jnp.where(early, own, other), jnp.where(early, other, own)], axis=1)

    row = lax.broadcasted_iota(jnp.int32, (traj, 2 * step), 0)
    lane = lax.broadcasted_iota(jnp.int32, (traj, 2 * step), 1)

    def column(ref):
        out = jnp.full((traj, 2 * step), ref[0])
        for i in range(1, traj):
            out = jnp.where(row == i, ref[i], out)
        return out

    keep = 1.0 - in_time(dones_ref[...], other_dones_ref[...]).astype(jnp.float32)
    length = column(lengths_ref)
    live = jnp.where(lane < length, 1.0, 0.0)
    coef = jnp.where(lane + 1 < length, column(discount_ref) * keep, 0.0)
    ready_ref[0] = in_time(rewards_ref[...], other_rewards_ref[...])
    ready_ref[1] = coef
    ready_ref[2] = coef * column(trace_ref)
    ready_ref[3] = live
    ready_ref[4] = jnp.full((traj, 2 * step), out_bias_ref[0])
    own_live_ref[...] = jnp.where(early, live[:, :step], live[:, step:])


def scan_kernel(part_ref, swapped_ref, ready_ref, returns_ref, gain_ref, stats_ref):
    traj, steps = returns_ref.shape
    step = steps // 2
    early = core_parity() == 0
    both = part_ref[...] + pltpu.roll(swapped_ref[...], 1, 0)
    first, second = jnp.where(early, both[0:1], both[1:2]), jnp.where(early, both[1:2], both[0:1])
    values = jnp.concatenate(
        [
            jnp.concatenate([x[:, i * step : (i + 1) * step] for i in range(traj)], axis=0) for x in (first, second)
        ],
        axis=1,
    )
    values = values + ready_ref[4]
    lane = lax.broadcasted_iota(jnp.int32, values.shape, 1)
    decay, live = ready_ref[2], ready_ref[3]
    following = pltpu.roll(values, steps - 1, 1)
    gain = live * (ready_ref[0] + ready_ref[1] * jnp.where(lane == steps - 1, 0.0, following) - values)
    span = 1
    while span < steps:
        inside = lane < steps - span
        gain = gain + decay * jnp.where(inside, pltpu.roll(gain, steps - span, 1), 0.0)
        if 2 * span < steps:
            decay = decay * jnp.where(inside, pltpu.roll(decay, steps - span, 1), 0.0)
        span *= 2
    count, total, squares = moments(gain, live)
    slot = lax.broadcasted_iota(jnp.int32, stats_ref.shape, 2)
    stats_ref[...] = jnp.where(slot == 0, count, jnp.where(slot == 1, total, squares))
    gain_ref[...] = gain
    returns_ref[...] = live * (gain + values)


def final_kernel(every_ref, gain_ref, live_ref, advantages_ref):
    step = advantages_ref.shape[1]
    gain = jnp.where(core_parity() == 0, gain_ref[:, :step], gain_ref[:, step:])
    advantages_ref[...] = normalized(every_ref[...], gain, live_ref[...])


PARAMS = pltpu.CompilerParams(vmem_limit_bytes=8 * 2**20)
VMEM = pl.BlockSpec(memory_space=pltpu.VMEM)
SMEM = pl.BlockSpec(memory_space=pltpu.SMEM)


def kept(x):
    return pltpu.with_memory_space_constraint(x, pltpu.VMEM)


def values_in_kernels(planes, calls, own_rows, other_rows, first_bias, second_weight):
    rows, half = own_rows.shape[0], first_bias.shape[0] // 2
    row_vectors = [x.reshape(1, 2 * half) for x in (first_bias, second_weight)]
    acc = pltpu.VMEM((2 * rows, half), jnp.float32)
    other_rows = kept(other_rows)
    own_rows, constants = pl.pallas_call(
        bring_kernel,
        out_shape=(pltpu.VMEM(own_rows.shape, own_rows.dtype), pltpu.VMEM((2, half), jnp.float32)),
        in_specs=[pl.BlockSpec(memory_space=pl.ANY)] * 3,
        out_specs=(VMEM,) * 2,
        scratch_shapes=[pltpu.SemaphoreType.DMA((3,))],
        compiler_params=PARAMS,
    )(own_rows, *row_vectors)
    own_rows, constants, pre = kept(own_rows), kept(constants), []
    for at, call in enumerate(calls):
        groups = [(kind, k, tuple(sorted(blocks))) for kind, k, blocks in call]
        weights = [kept(blocks[i]) for _, _, blocks in call for i in sorted(blocks)]
        if at + 1 < len(calls):
            pre = [
                pl.pallas_call(
                    functools.partial(dot_kernel, groups, planes, not pre),
                    out_shape=acc,
                    in_specs=[VMEM] * (2 + len(weights) + len(pre)),
                    out_specs=VMEM,
                    input_output_aliases={2 + len(weights): 0} if pre else {},
                    compiler_params=PARAMS,
                )(own_rows, other_rows, *weights, *pre)
            ]
        else:
            part = pl.pallas_call(
                functools.partial(value_kernel, groups, planes),
                out_shape=pltpu.VMEM((2, rows), jnp.float32),
                in_specs=[VMEM] * (4 + len(weights)),
                out_specs=VMEM,
                scratch_shapes=[acc],
                compiler_params=PARAMS,
            )(own_rows, other_rows, *weights, *pre, constants)
    return part


def on_device(hidden, first_weight, first_bias, second_weight, second_bias, rewards, dones, lengths, discount, trace):
    dp_size, tm_size = lax.axis_size("dp"), lax.axis_size("tm")
    traj, step, feature_count = hidden.shape
    shard, unit_count = first_weight.shape
    half = unit_count // 2
    rows = traj * step
    devices = dp_size * tm_size
    planes = dp_size // 4
    order, place = ring_places(planes)
    first, second, up, down = routes(dp_size, tm_size)
    pair = [(i, i ^ 1) for i in range(tm_size)]
    parity = core_parity()

    own = lax.dynamic_slice(first_weight, (0, parity * half), (shard, half))
    other_hidden = lax.ppermute(hidden, "tm", pair)

    def sent(block, route):
        return lax.ppermute(block, BOTH, route)

    half_way = planes // 2
    near, far = {}, {}
    for way, route, turns in (("up", up, range(half_way + 1)), ("down", down, range(planes - 1, half_way, -1))):
        piece = own
        for k in turns:
            if k:
                piece = sent(piece, route)
            if k < 2 or way == "down":
                beside = sent(piece, first)
            else:
                beside = sent(beside, route)
            near[k] = (piece, beside)
            far[k] = (sent(piece, second), sent(beside, second))
    sequence = [0, 1] + list(range(planes - 1, half_way, -1)) + list(range(2, half_way + 1))
    calls, last = [[("near", 0, dict(enumerate(near[0])))]], 0
    for k in sequence[1:]:
        calls.append([("near", k, dict(enumerate(near[k]))), ("far", last, dict(enumerate(far[last])))])
        last = k
    calls.append([("far", last, dict(enumerate(far[last])))])

    other_rewards = lax.ppermute(rewards, "tm", pair)
    other_dones = lax.ppermute(dones, "tm", pair)

    own_rows, other_rows = hidden.reshape(rows, feature_count), other_hidden.reshape(rows, feature_count)
    if shard % 128 == 0 and rows % 128 == 0:
        part = values_in_kernels(planes, calls, own_rows, other_rows, first_bias, second_weight)
    else:
        pre = jnp.zeros((2 * rows, half), jnp.float32)
        for kind, k, blocks in sum(calls, []):
            for i, at in enumerate(columns_of(kind, k, planes, shard)):
                columns = [lax.dynamic_slice(x, (0, at), (rows, shard)) for x in (own_rows, other_rows)]
                pre = pre + jnp.dot(jnp.concatenate(columns), blocks[i], preferred_element_type=jnp.float32)
        bias, out_weight = (lax.dynamic_slice(x, (parity * half,), (half,)) for x in (first_bias, second_weight))
        part = jnp.sum(jax.nn.silu(pre + bias) * out_weight, axis=1).reshape(2, rows)
    swapped = lax.ppermute(part, "tm", pair)
    block = jax.ShapeDtypeStruct((traj, step), jnp.float32)
    pair_block = jax.ShapeDtypeStruct((traj, 2 * step), jnp.float32)
    if tm_size == 2:
        ready, own_live = pl.pallas_call(
            prepare_kernel,
            out_shape=(pltpu.VMEM((5, *pair_block.shape), jnp.float32), pltpu.VMEM(block.shape, jnp.float32)),
            in_specs=[VMEM] * 4 + [SMEM] * 4,
            out_specs=(VMEM,) * 2,
            compiler_params=PARAMS,
        )(rewards, other_rewards, dones, other_dones, lengths, discount, trace, second_bias)
        returns, gain, stats = pl.pallas_call(
            scan_kernel,
            out_shape=(
                pltpu.VMEM(pair_block.shape, jnp.float32),
                pltpu.VMEM(pair_block.shape, jnp.float32),
                pltpu.VMEM((devices, 1, 128), jnp.float32),
            ),
            in_specs=[VMEM] * 3,
            out_specs=(VMEM,) * 3,
            compiler_params=PARAMS,
        )(kept(part), kept(swapped), kept(ready))
    else:

        def in_time(own, other):
            early = parity == 0
            return jnp.concatenate([jnp.where(early, own, other), jnp.where(early, other, own)], axis=1)

        values = (part + swapped[::-1] + second_bias[0]).reshape(2, traj, step)
        values = in_time(values[0], values[1])
        time_index = (lax.axis_index("tm") - parity) * step + jnp.arange(2 * step, dtype=jnp.int32)
        live = (time_index[None, :] < lengths[:, None]).astype(jnp.float32)
        live_next = ((time_index + 1)[None, :] < lengths[:, None]).astype(jnp.float32)
        coef = discount[:, None] * (1.0 - in_time(dones, other_dones).astype(jnp.float32)) * live_next
        following = jnp.concatenate([values[:, 1:], passed_along(values[:, :1], "tm", -2)], axis=1)
        delta = live * (in_time(rewards, other_rewards) + coef * following - values)
        decay = coef * trace[:, None]
        product_to_end, offset = lax.associative_scan(pair_combine, (decay, delta), reverse=True, axis=1)
        incoming = jnp.zeros((traj,), jnp.float32)
        for _ in range(tm_size // 2 - 1):
            incoming = passed_along(offset[:, 0] + product_to_end[:, 0] * incoming, "tm", -2)
        gain = offset + product_to_end * incoming[:, None]
        slot = jnp.arange(128)
        count, total, squares = moments(gain, live)
        stats = jnp.where(slot == 0, count, jnp.where(slot == 1, total, squares))
        stats = jnp.broadcast_to(stats, (devices, 1, 128))
        returns = live * (gain + values)
    every = lax.all_to_all(stats, BOTH, 0, 0, tiled=True).reshape(devices, 128)
    returns = lax.dynamic_slice(returns, (0, parity * step), (traj, step))
    if tm_size == 2:
        advantages = pl.pallas_call(
            final_kernel, out_shape=block, in_specs=[VMEM] * 3, out_specs=VMEM, compiler_params=PARAMS
        )(every, kept(gain), kept(own_live))
    else:
        gain, live = (lax.dynamic_slice(x, (0, parity * step), (traj, step)) for x in (gain, live))
        advantages = normalized(every, gain, live)
    return (advantages, returns)


def solution(mesh):
    in_specs = (
        P("dp", "tm", None),
        P("dp", None),
        P(),
        P(),
        P(),
        P("dp", "tm"),
        P("dp", "tm"),
        P("dp"),
        P("dp"),
        P("dp"),
    )
    out_specs = (P("dp", "tm"), P("dp", "tm"))


    return jax.shard_map(on_device, mesh=mesh, in_specs=in_specs, out_specs=out_specs, check_vma=False)
```
